32 devices in a mesh: fsdp: 16 (over z, y, x), model: 2 (over core).
Axes of the slice: x: 2, y: 2, z: 4, core: 2. Of those that a mesh axis runs over, the one named last changes fastest.
Arguments:
- train_query: float32 [2560, 4096], P('fsdp', 'model'), may hold values from -0.15625 to 0.15625
- drift_query: float32 [2560, 4096], P('fsdp', 'model'), may hold values from -6 to 6
- spread_query: float32 [2560, 4096], P('fsdp', 'model'), may hold values from 0.1 to 10
- train_key: float32 [2560, 1024], P('fsdp', 'model'), may hold values from -0.15625 to 0.15625
- drift_key: float32 [2560, 1024], P('fsdp', 'model'), may hold values from -6 to 6
- spread_key: float32 [2560, 1024], P('fsdp', 'model'), may hold values from 0.1 to 10
- train_value: float32 [2560, 1024], P('fsdp', 'model'), may hold values from -0.15625 to 0.15625
- drift_value: float32 [2560, 1024], P('fsdp', 'model'), may hold values from -6 to 6
- spread_value: float32 [2560, 1024], P('fsdp', 'model'), may hold values from 0.1 to 10
- norm_train: float32 [2560], P(('fsdp', 'model')), may hold values from 0.25 to 1.75
- norm_step: float32 [2560], P(('fsdp', 'model')), may hold values from -0.3 to 0.3
Outputs:
- serve_query: bfloat16 [2560, 4096], P(None, 'model')
- serve_key: bfloat16 [2560, 1024], P(None, 'model')
- serve_value: bfloat16 [2560, 1024], P(None, 'model')
- factor_query: float32 [4096], P('model')
- factor_key: float32 [1024], P('model')
- factor_value: float32 [1024], P('model')
- serve_norm: bfloat16 [2560], replicated
- fresh_query: float32 [2560, 4096], P('fsdp', 'model')
- fresh_key: float32 [2560, 1024], P('fsdp', 'model')
- fresh_value: float32 [2560, 1024], P('fsdp', 'model')
The draws below stay inside these ranges and needn't reach their ends.
All inputs are finite; a program needn't handle non-finite values. Where the reference program divides by a largest or mean magnitude, that divisor is 1e-20 or more.
Results may differ from the reference program's by a relative error of at most 0.001.
Values may be sent and summed in bfloat16 or wider, within the bound.
A program may use at most 64 MiB of HBM per device.

```python
import math
import jax
import jax.numpy as jnp
from jax import lax

D_MODEL = 2560
Q_DIM = 4096
KV_DIM = 1024


def raised(result, rng, source, target, parts, factor):
    owner, partner = [(jnp.arange(result.shape[dim]) // (result.shape[dim] // parts)).reshape([-1 if axis == dim else 1 for axis in range(result.ndim)]) for dim in (source, target)]
    chosen = jax.random.permutation(rng, parts)[partner]
    strong = (owner == chosen) | (owner == (partner + parts // 2) % parts)
    return jnp.where(strong, factor * result, result)


def block_scale(rng, dims, pieces, low, high):
    factor_of = 1.0
    for axis_at, shards_of in pieces:
        draws = jax.random.uniform(jax.random.fold_in(jax.random.fold_in(rng, 6), axis_at), (shards_of,), jnp.float32, low / len(pieces), high / len(pieces))
        factor_of = factor_of * jnp.repeat(jnp.exp(draws), dims[axis_at] // shards_of).reshape((-1,) + (1,) * (len(dims) - 1 - axis_at))
    return factor_of


def scatter_about(stream_key, extent, spread, bound, shards=(), dtype=jnp.bfloat16):
    drawn = jax.random.normal(stream_key, extent, jnp.float32) * spread
    if len(shards) > 0:
        drawn = block_scale(stream_key, extent, shards, -0.22, 0.18) * drawn
    return jnp.clip(drawn, min=-bound, max=bound).astype(dtype)


def gaussian_with(own_key, extent, deviation, limit, split, heavy, kind=jnp.bfloat16):
    entries = deviation * jax.random.normal(own_key, extent, jnp.float32)
    if split:
        entries = entries * block_scale(own_key, extent, split, -0.22, 0.18)
    return jnp.clip(raised(entries, jax.random.fold_in(own_key, 3), *heavy), -limit, limit).astype(kind)


def setup_inputs(seed: int = 0) -> dict:
    arg_keys = jax.random.split(jax.random.key(seed), 12)
    train_query = gaussian_with(arg_keys[0], (D_MODEL, Q_DIM), D_MODEL ** -0.5, 0.15625, ((0, 16), (1, 2)), (0, 1, 16, 2.0), jnp.float32)
    drift_query = scatter_about(arg_keys[1], (D_MODEL, Q_DIM), 1.0, 6.0, ((0, 16), (1, 2)), jnp.float32)
    spread_query = jnp.clip(jnp.exp(math.log(10.0) - 4.6051702 * jax.random.uniform(arg_keys[2], (D_MODEL, Q_DIM), jnp.float32) ** block_scale(arg_keys[2], (D_MODEL, Q_DIM), ((0, 16), (1, 2)), -0.2, 0.2)), 0.1, 10.0)
    train_key = gaussian_with(arg_keys[3], (D_MODEL, KV_DIM), D_MODEL ** -0.5, 0.15625, ((0, 16), (1, 2)), (0, 1, 16, 2.0), jnp.float32)
    drift_key = scatter_about(arg_keys[4], (D_MODEL, KV_DIM), 1.0, 6.0, ((0, 16), (1, 2)), jnp.float32)
    spread_key = jnp.clip(jnp.exp(math.log(10.0) - 4.6051702 * jax.random.uniform(arg_keys[5], (D_MODEL, KV_DIM), jnp.float32) ** block_scale(arg_keys[5], (D_MODEL, KV_DIM), ((0, 16), (1, 2)), -0.2, 0.2)), 0.1, 10.0)
    train_value = gaussian_with(arg_keys[6], (D_MODEL, KV_DIM), D_MODEL ** -0.5, 0.15625, ((0, 16), (1, 2)), (0, 1, 16, 2.0), jnp.float32)
    drift_value = scatter_about(arg_keys[7], (D_MODEL, KV_DIM), 1.0, 6.0, ((0, 16), (1, 2)), jnp.float32)
    spread_value = jnp.clip(jnp.exp(math.log(10.0) - 4.6051702 * jax.random.uniform(arg_keys[8], (D_MODEL, KV_DIM), jnp.float32) ** block_scale(arg_keys[8], (D_MODEL, KV_DIM), ((0, 16), (1, 2)), -0.2, 0.2)), 0.1, 10.0)
    norm_train = jnp.clip(1.0 + 0.15 * jax.random.normal(arg_keys[9], (D_MODEL,), jnp.float32), 0.25, 1.75)
    norm_step = jnp.clip(jax.random.uniform(arg_keys[10], (D_MODEL,), jnp.float32, -0.3, 0.3) * block_scale(arg_keys[10], (D_MODEL,), ((0, 32),), -0.4, 0.0), -0.3, 0.3)
    return dict(train_query=train_query, drift_query=drift_query, spread_query=spread_query, train_key=train_key, drift_key=drift_key, spread_key=spread_key, train_value=train_value, drift_value=drift_value, spread_value=spread_value, norm_train=norm_train, norm_step=norm_step)


learn_rate = 0.02
decay_rate = 0.05
tiny_value = 1e-08

def reference(train_query, drift_query, spread_query, train_key, drift_key, spread_key, train_value, drift_value, spread_value, norm_train, norm_step):
    fresh_query = train_query - learn_rate * (drift_query / (jnp.sqrt(spread_query) + tiny_value) + decay_rate * train_query)
    fresh_key = train_key - learn_rate * (drift_key / (jnp.sqrt(spread_key) + tiny_value) + decay_rate * train_key)
    fresh_value = train_value - learn_rate * (drift_value / (jnp.sqrt(spread_value) + tiny_value) + decay_rate * train_value)
    factor_query = lax.optimization_barrier(jnp.max(jnp.abs(fresh_query), axis=0))
    serve_query = (fresh_query / factor_query).astype(jnp.bfloat16)
    factor_key = lax.optimization_barrier(jnp.max(jnp.abs(fresh_key), axis=0))
    serve_key = (fresh_key / factor_key).astype(jnp.bfloat16)
    factor_value = lax.optimization_barrier(jnp.max(jnp.abs(fresh_value), axis=0))
    serve_value = (fresh_value / factor_value).astype(jnp.bfloat16)
    serve_norm = (norm_train + norm_step).astype(jnp.bfloat16)
    return (serve_query, serve_key, serve_value, factor_query, factor_key, factor_value, serve_norm, fresh_query, fresh_key, fresh_value)
```

```python
import functools
import math

import jax
import jax.numpy as jnp
from jax import lax
from jax.experimental import pallas as pl
from jax.experimental.pallas import tpu as pltpu
from jax.sharding import PartitionSpec as P

learn_rate = 0.02
decay_rate = 0.05
tiny_value = 1e-08
MESH = pl.DeviceIdType.MESH
ROWS = 16
CHUNK = 32
VMEM_BYTES = 67043328
LANES = 128

AZ, BZ, AX, AY, BXF, BYF, DIAG, COUNT = 0, 4, 20, 24, 28, 29, 30, 31
TO_X, TO_Y, INWARD, OUTWARD = 0, 1, 2, 3


def stepped(train, drift, spread):
    return train - learn_rate * (drift / (jnp.sqrt(spread) + tiny_value) + decay_rate * train)


def gather_kernel(
    part_a, widths,
    tq, dq, sq, tk, dk, sk, tv, dv, sv, norm_train, norm_step,
    held, fresh, factor, norms,
    local, norm_in, top, early,
    mx, in_sem, norm_sem, mx_send, mx_recv, nm_send, nm_recv, early_send, early_recv, send, recv,
):
    f = lax.axis_index("fsdp")
    m = lax.axis_index("model")
    z = f // 4
    r = f % 4
    y = r // 2
    x = r % 2
    rx, ry, rd = y * 2 + (1 - x), (1 - y) * 2 + x, (1 - y) * 2 + (1 - x)
    n, rows, width = held.shape
    starts = (0, widths[0], widths[0] + widths[1])
    inputs = ((tq, dq, sq), (tk, dk, sk), (tv, dv, sv))
    half_a = part_a // 2
    half_b = (rows - part_a) // 2

    def device(zz, rr):
        return {"fsdp": zz * 4 + rr, "model": m}

    plane = [device(z, rx), device(z, ry), device(z, rd)]
    line = [device((z + k) % 4, r) for k in range(1, 4)]
    partner = {"fsdp": f, "model": 1 - m}

    barrier = pltpu.get_barrier_semaphore()
    for peer in plane + line + [partner]:
        pl.semaphore_signal(barrier, inc=1, device_id=peer, device_id_type=MESH)

    def part(i):
        return pl.ds(pl.multiple_of(i * CHUNK, CHUNK), CHUNK)

    for i in range(rows // CHUNK):
        for a in range(3):
            cols = pl.ds(starts[a], widths[a])
            for k, src in enumerate(inputs[a]):
                pltpu.make_async_copy(src.at[part(i)], local.at[k, part(i), cols], in_sem.at[i]).start()
    norm_loads = [
        pltpu.make_async_copy(src, norm_in.at[k], norm_sem.at[k])
        for k, src in enumerate((norm_train, norm_step))
    ]
    for copy in norm_loads:
        copy.start()

    top[...] = jnp.zeros_like(top)
    step = math.gcd(512, width)

    def chunk(i, carry):
        whole = local.at[:, part(i)]
        pltpu.make_async_copy(whole, whole, in_sem.at[i]).wait()
        for c in range(0, width, step):
            cols = slice(c, c + step)
            best = top[:, cols]
            for g in range(CHUNK // 8):
                at = pl.ds(pl.multiple_of(i * CHUNK + g * 8, 8), 8)
                new = stepped(local[0, at, cols], local[1, at, cols], local[2, at, cols])
                fresh[at, cols] = new
                best = jnp.maximum(best, jnp.abs(new))
            top[:, cols] = best
        return carry

    lax.fori_loop(0, rows // CHUNK, chunk, 0)
    mx[0] = jnp.max(top[...], axis=0, keepdims=True)
    for copy in norm_loads:
        copy.wait()
    norms[m, f] = jnp.zeros_like(norms[m, f])
    norms[m, f, :, : norm_in.shape[2]] = norm_in[0] + norm_in[1]

    pl.semaphore_wait(barrier, 7)

    def remote(src, dst, s, d, peer):
        return pltpu.make_async_remote_copy(
            src_ref=src, dst_ref=dst, send_sem=s, recv_sem=d, device_id=peer, device_id_type=MESH
        )

    for k, peer in enumerate(plane):
        remote(mx.at[0], mx.at[1 + k], mx_send.at[0], mx_recv.at[0], peer).start()
    mine = norms.at[m, f]
    for peer in plane:
        remote(mine, mine, nm_send.at[0], nm_recv.at[0], peer).start()
    for k in range(2):
        remote(fresh.at[pl.ds(part_a, rows - part_a)], early.at[k], early_send.at[0], early_recv.at[k], plane[k]).start()
    got_mx = mx.at[pl.ds(1, 3)]
    remote(got_mx, got_mx, mx_send.at[0], mx_recv.at[0], plane[0]).wait_recv()
    mx[4] = jnp.maximum(jnp.maximum(mx[0], mx[1]), jnp.maximum(mx[2], mx[3]))
    for k, peer in enumerate(line):
        remote(mx.at[4], mx.at[5 + k], mx_send.at[0], mx_recv.at[1], peer).start()
    got_nm = norms.at[m, pl.ds(0, 3)]
    remote(got_nm, got_nm, nm_send.at[0], nm_recv.at[0], plane[0]).wait_recv()
    group = norms.at[m, pl.ds(z * 4, 4)]
    for peer in line:
        remote(group, group, nm_send.at[0], nm_recv.at[1], peer).start()
    remote(got_mx, got_mx, mx_send.at[0], mx_recv.at[1], plane[0]).wait_recv()
    factor[...] = jnp.maximum(jnp.maximum(mx[4], mx[5]), jnp.maximum(mx[6], mx[7]))

    def narrow(ref, skip, block, first, last):
        def body(i, carry):
            at = pl.ds(pl.multiple_of(first + i * ROWS, ROWS), ROWS)
            here = pl.ds(pl.multiple_of(first - skip + i * ROWS, ROWS), ROWS)
            for c in range(0, width, step):
                cols = slice(c, c + step)
                held[block, at, cols] = (ref[here, cols] / factor[:, cols]).astype(jnp.bfloat16)
            return carry
        lax.fori_loop(0, (last - first) // ROWS, body, 0)

    def go(zz, rr, first, last, way, d, peer):
        block = held.at[zz * 4 + rr, pl.ds(first, last - first)]
        remote(block, block, send.at[way], recv.at[d], peer).start()

    def got(zz, rr, first, last, d):
        block = held.at[zz * 4 + rr, pl.ds(first, last - first)]
        remote(block, block, send.at[0], recv.at[d], plane[0]).wait_recv()

    def span(count):
        for blocks in range(1, n + 1):
            if count % (blocks * 8) == 0 and count // blocks <= rows:
                return held.at[pl.ds(0, blocks), pl.ds(0, count // blocks)]
        raise ValueError(count)

    def sent(way, count):
        all_of = span(count)
        remote(all_of, all_of, send.at[way], recv.at[0], plane[0]).wait_send()

    hi = z // 2
    z_end, z_mid, z_mid2, z_end2 = 3 * hi, 1 + hi, 2 - hi, 3 - 3 * hi
    is_end = z == z_end
    is_mid = z == z_mid
    near = z_end + z_mid - z
    plane_of = (r, rx, ry, rd)

    def az(zz, to, outward):
        go(zz, r, 0, part_a, OUTWARD if outward else INWARD, AZ + zz, device(to, r))

    def bz(zz, j, to, outward):
        go(zz, plane_of[j], part_a, rows, OUTWARD if outward else INWARD, BZ + zz * 4 + j, device(to, r))

    def got_az(zz):
        got(zz, r, 0, part_a, AZ + zz)

    def got_bz(zz, j):
        got(zz, plane_of[j], part_a, rows, BZ + zz * 4 + j)

    def a_own(zz):
        go(zz, r, 0, part_a, TO_X, AX + zz, plane[0])
        go(zz, r, 0, part_a, TO_Y, AY + zz, plane[1])

    def a_forward(zz):
        got(zz, rx, 0, part_a, AX + zz)
        go(zz, rx, half_a, part_a, TO_Y, DIAG, plane[1])
        got(zz, ry, 0, part_a, AY + zz)
        go(zz, ry, 0, half_a, TO_X, DIAG, plane[0])

    narrow(fresh, 0, f, 0, part_a)

    @pl.when(is_end)
    def _():
        az(z_end, z_mid, False)

    @pl.when(is_mid)
    def _():
        az(z_mid, z_mid2, False)
        az(z_mid, z_end, True)

    a_own(z)
    narrow(fresh, 0, f, part_a, rows)
    for k, rr in enumerate((rx, ry)):
        remote(early.at[k], early.at[k], early_send.at[0], early_recv.at[k], plane[k]).wait_recv()
        narrow(early.at[k], part_a, z * 4 + rr, part_a, rows)
        if k == 0:
            go(z, rx, part_a + half_b, rows, TO_Y, BYF, plane[1])
    go(z, ry, part_a, part_a + half_b, TO_X, BXF, plane[0])

    @pl.when(is_end)
    def _():
        for j in (0, 1):
            bz(z_end, j, z_mid, False)
        got_az(z_mid)

    @pl.when(is_mid)
    def _():
        for j in (0, 1):
            bz(z_mid, j, z_mid2, False)
            bz(z_mid, j, z_end, True)
        got_az(z_end)
        az(z_end, z_mid2, False)
        got_az(z_mid2)
        az(z_mid2, z_end, True)

    a_own(near)
    got(z, rd, part_a, part_a + half_b, BXF)
    got(z, rd, part_a + half_b, rows, BYF)

    @pl.when(is_end)
    def _():
        for j in (2, 3):
            bz(z_end, j, z_mid, False)

    @pl.when(is_mid)
    def _():
        for j in (2, 3):
            bz(z_mid, j, z_mid2, False)
            bz(z_mid, j, z_end, True)

    a_forward(z)

    @pl.when(is_end)
    def _():
        got_az(z_mid2)

    a_own(z_mid2)

    @pl.when(is_mid)
    def _():
        got_az(z_end2)
        az(z_end2, z_end, True)

    a_forward(near)

    @pl.when(is_mid)
    def _():
        for j in range(4):
            got_bz(z_end, j)
            bz(z_end, j, z_mid2, False)
        for j in range(4):
            got_bz(z_mid2, j)
            bz(z_mid2, j, z_end, True)

    @pl.when(is_end)
    def _():
        got_az(z_end2)

    a_own(z_end2)
    a_forward(z_mid2)

    @pl.when(is_mid)
    def _():
        for j in range(4):
            got_bz(z_end2, j)
            bz(z_end2, j, z_end, True)

    got_nm = norms.at[m, pl.ds(0, 12)]
    remote(got_nm, got_nm, nm_send.at[0], nm_recv.at[1], plane[0]).wait_recv()
    whole = norms.at[m]
    remote(whole, whole, nm_send.at[1], nm_recv.at[2], partner).start()

    a_forward(z_end2)

    @pl.when(is_end)
    def _():
        for zz in (z_mid, z_mid2, z_end2):
            for j in range(4):
                got_bz(zz, j)

    diagonal = span(4 * part_a)
    remote(diagonal, diagonal, send.at[0], recv.at[DIAG], plane[0]).wait_recv()
    theirs = norms.at[1 - m]
    remote(theirs, theirs, nm_send.at[1], nm_recv.at[2], partner).wait_recv()
    sums = mx.at[pl.ds(0, 6)]
    remote(sums, sums, mx_send.at[0], mx_recv.at[0], plane[0]).wait_send()
    tags = norms.at[m, pl.ds(0, 15)]
    remote(tags, tags, nm_send.at[0], nm_recv.at[0], plane[0]).wait_send()
    remote(theirs, theirs, nm_send.at[1], nm_recv.at[2], partner).wait_send()
    remote(early, early, early_send.at[0], early_recv.at[0], plane[0]).wait_send()
    sent(TO_X, 4 * (part_a + half_a) + half_b)
    sent(TO_Y, 4 * (part_a + part_a - half_a) + rows - part_a - half_b)
    up = part_a + 4 * (rows - part_a)

    @pl.when(is_end)
    def _():
        sent(INWARD, up)

    @pl.when(is_mid)
    def _():
        sent(INWARD, 2 * up)
        sent(OUTWARD, 3 * up)


def write_kernel(length, held, fresh, factor, norms, *rest):
    serve, rates, fresh_out, norm_out, flat, norm_row, sems = rest[:3], rest[3:6], rest[6:9], *rest[9:]
    n = held.shape[0]
    cut = max(1, n // 4)
    copies = []
    start = 0
    for k in range(3):
        cols = pl.ds(start, serve[k].shape[2])
        for b in range(0, n, cut):
            copies.append((held.at[pl.ds(b, cut), :, cols], serve[k].at[pl.ds(b, cut)]))
        copies.append((factor.at[:, cols], rates[k]))
        copies.append((fresh.at[:, cols], fresh_out[k]))
        start += serve[k].shape[2]
    copies = [pltpu.make_async_copy(src, dst, sems.at[i]) for i, (src, dst) in enumerate(copies)]
    for copy in copies:
        copy.start()
    at = 0
    for b in range(n):
        for c in range(norms.shape[0]):
            flat[:, at : at + length] = norms[c, b, :, :length]
            at += length
    norm_row[...] = flat[...].astype(jnp.bfloat16).reshape(at)
    last = pltpu.make_async_copy(norm_row, norm_out, sems.at[len(copies)])
    last.start()
    for copy in copies:
        copy.wait()
    last.wait()


def with_kernel(part_a, *args):
    (tq, dq, sq, tk, dk, sk, tv, dv, sv, norm_train, norm_step) = args
    length = norm_train.shape[0]
    padded = -(-length // LANES) * LANES
    n, cores = lax.axis_size("fsdp"), lax.axis_size("model")
    rows = tq.shape[0]
    widths = (tq.shape[1], tk.shape[1], tv.shape[1])
    width = sum(widths)
    vmem = pl.BlockSpec(memory_space=pltpu.VMEM)
    hbm = pl.BlockSpec(memory_space=pltpu.HBM)
    f32, bf16 = jnp.float32, jnp.bfloat16
    room = VMEM_BYTES - n * rows * width * 2 - rows * width * 4 - 192 * 1024
    held, fresh, factor, norms = pl.pallas_call(
        functools.partial(gather_kernel, part_a, widths),
        out_shape=(
            pltpu.VMEM((n, rows, width), bf16),
            pltpu.VMEM((rows, width), f32),
            pltpu.VMEM((1, width), f32),
            pltpu.VMEM((cores, n, 1, padded), f32),
        ),
        in_specs=[hbm] * 11,
        out_specs=(vmem,) * 4,
        scratch_shapes=[
            pltpu.VMEM((3, rows, width), f32),
            pltpu.VMEM((2, 1, length), f32),
            pltpu.VMEM((8, width), f32),
            pltpu.VMEM((2, rows - part_a, width), f32),
            pltpu.VMEM((8, 1, width), f32),
            pltpu.SemaphoreType.DMA((rows // CHUNK,)),
            pltpu.SemaphoreType.DMA((2,)),
            pltpu.SemaphoreType.DMA((1,)),
            pltpu.SemaphoreType.DMA((2,)),
            pltpu.SemaphoreType.DMA((2,)),
            pltpu.SemaphoreType.DMA((3,)),
            pltpu.SemaphoreType.DMA((1,)),
            pltpu.SemaphoreType.DMA((2,)),
            pltpu.SemaphoreType.DMA((4,)),
            pltpu.SemaphoreType.DMA((COUNT,)),
        ],
        compiler_params=pltpu.CompilerParams(
            collective_id=0, has_side_effects=True, vmem_limit_bytes=room
        ),
        name="gather",
    )(
        tq, dq, sq, tk, dk, sk, tv, dv, sv,
        norm_train.reshape(1, length), norm_step.reshape(1, length),
    )
    out = pl.pallas_call(
        functools.partial(write_kernel, length),
        out_shape=(
            *[jax.ShapeDtypeStruct((n, rows, w), bf16) for w in widths],
            *[jax.ShapeDtypeStruct((1, w), f32) for w in widths],
            *[jax.ShapeDtypeStruct((rows, w), f32) for w in widths],
            jax.ShapeDtypeStruct((n * cores * length,), bf16),
        ),
        in_specs=[vmem] * 4,
        out_specs=(hbm,) * 10,
        scratch_shapes=[
            pltpu.VMEM((1, n * cores * length), f32),
            pltpu.VMEM((n * cores * length,), bf16),
            pltpu.SemaphoreType.DMA((19,)),
        ],
        compiler_params=pltpu.CompilerParams(vmem_limit_bytes=4 * 1024 * 1024),
        name="write",
    )(held, fresh, factor, norms)
    return (
        *[a.reshape(n * rows, w) for a, w in zip(out[:3], widths)],
        *[a.reshape(w) for a, w in zip(out[3:6], widths)],
        out[9], *out[6:9],
    )


def per_device(
    train_query,
    drift_query,
    spread_query,
    train_key,
    drift_key,
    spread_key,
    train_value,
    drift_value,
    spread_value,
    norm_train,
    norm_step,
):
    n, cores, rows = lax.axis_size("fsdp"), lax.axis_size("model"), train_query.shape[0]
    part_a = rows - (rows * 2 // 9 // (2 * ROWS)) * 2 * ROWS
    lanes_ok = all(a.shape[1] % LANES == 0 for a in (train_query, train_key, train_value))
    if n == 16 and cores == 2 and rows % CHUNK == 0 and part_a < rows and lanes_ok:
        return with_kernel(
            part_a,
            train_query, drift_query, spread_query,
            train_key, drift_key, spread_key,
            train_value, drift_value, spread_value,
            norm_train, norm_step,
        )
    fresh_query = train_query - learn_rate * (
        drift_query / (jnp.sqrt(spread_query) + tiny_value) + decay_rate * train_query
    )
    fresh_key = train_key - learn_rate * (
        drift_key / (jnp.sqrt(spread_key) + tiny_value) + decay_rate * train_key
    )
    fresh_value = train_value - learn_rate * (
        drift_value / (jnp.sqrt(spread_value) + tiny_value) + decay_rate * train_value
    )
    factor_query, factor_key, factor_value = lax.pmax(
        (
            jnp.max(jnp.abs(fresh_query), axis=0),
            jnp.max(jnp.abs(fresh_key), axis=0),
            jnp.max(jnp.abs(fresh_value), axis=0),
        ),
        "fsdp",
    )
    narrow_query, narrow_key, narrow_value = (
        (fresh_query / factor_query).astype(jnp.bfloat16),
        (fresh_key / factor_key).astype(jnp.bfloat16),
        (fresh_value / factor_value).astype(jnp.bfloat16),
    )
    serve_query, serve_key, serve_value = (
        lax.all_gather(narrow_query, "fsdp", axis=0, tiled=True),
        lax.all_gather(narrow_key, "fsdp", axis=0, tiled=True),
        lax.all_gather(narrow_value, "fsdp", axis=0, tiled=True),
    )
    serve_norm = lax.all_gather(
        (norm_train + norm_step).astype(jnp.bfloat16), ("fsdp", "model"), axis=0, tiled=True
    )
    return (
        serve_query,
        serve_key,
        serve_value,
        factor_query,
        factor_key,
        factor_value,
        serve_norm,
        fresh_query,
        fresh_key,
        fresh_value,
    )


def solution(mesh):
    in_specs = (
        P("fsdp", "model"),
        P("fsdp", "model"),
        P("fsdp", "model"),
        P("fsdp", "model"),
        P("fsdp", "model"),
        P("fsdp", "model"),
        P("fsdp", "model"),
        P("fsdp", "model"),
        P("fsdp", "model"),
        P(("fsdp", "model")),
        P(("fsdp", "model")),
    )
    out_specs = (
        P(None, "model"),
        P(None, "model"),
        P(None, "model"),
        P("model"),
        P("model"),
        P("model"),
        P(),
        P("fsdp", "model"),
        P("fsdp", "model"),
        P("fsdp", "model"),
    )
    return jax.shard_map(
        per_device, mesh=mesh, in_specs=in_specs, out_specs=out_specs, check_vma=False
    )
```

```python
import functools
import math

import jax
import jax.numpy as jnp
from jax import lax
from jax.experimental import pallas as pl
from jax.experimental.pallas import tpu as pltpu
from jax.sharding import PartitionSpec as P

learn_rate = 0.02
decay_rate = 0.05
tiny_value = 1e-08
MESH = pl.DeviceIdType.MESH
ROWS = 8
SUB = 8
CHUNK = 32
VMEM_BYTES = 67043328
LANES = 128

AZ, BZ, AX, AY, BXF, BYF, DIAG, BX, BY, COUNT = 0, 4, 20, 24, 28, 29, 30, 31, 32, 33
EARLY, FIRST, LEAD = 16, 8, 6
AX_SENT, AY_SENT, FX_SENT, FY_SENT, BX_SENT, BY_SENT, IN_A, IN_B, OUT_A, OUT_B, KINDS = range(11)


def stepped(train, drift, spread):
    return train - learn_rate * (drift / (jnp.sqrt(spread) + tiny_value) + decay_rate * train)


def cover(count, blocks, down, across):
    for c in range(across, 0, -1):
        for b in range(1, blocks + 1):
            if count % (b * c) == 0 and count // (b * c) <= down:
                return b, count // (b * c), c
    raise ValueError("no cover")


def gather_kernel(
    part_a, split, widths,
    tq, dq, sq, tk, dk, sk, tv, dv, sv, norm_train, norm_step,
    held, fresh, factor, norms,
    local, norm_in, top, early,
    mx, lead_sem, in_sem, norm_sem, mx_send, mx_recv, nm_send, nm_recv, early_send, early_recv, send, recv,
):
    f = lax.axis_index("fsdp")
    m = lax.axis_index("model")
    z = f // 4
    r = f % 4
    y = r // 2
    x = r % 2
    rx, ry, rd = y * 2 + (1 - x), (1 - y) * 2 + x, (1 - y) * 2 + (1 - x)
    n, rows, width = held.shape
    starts = (0, widths[0], widths[0] + widths[1])
    inputs = ((tq, dq, sq), (tk, dk, sk), (tv, dv, sv))
    low, high = part_a

    def device(zz, rr):
        return {"fsdp": zz * 4 + rr, "model": m}

    plane = [device(z, rx), device(z, ry), device(z, rd)]
    line = [device((z + k) % 4, r) for k in range(1, 4)]
    partner = {"fsdp": f, "model": 1 - m}

    barrier = pltpu.get_barrier_semaphore()
    for peer in plane + line + [partner]:
        pl.semaphore_signal(barrier, inc=1, device_id=peer, device_id_type=MESH)

    def part(i):
        return pl.ds(pl.multiple_of(i * CHUNK, CHUNK), CHUNK)

    lead, rest = pl.ds(0, split), pl.ds(split, width - split)
    last = rows // CHUNK - 1
    for k, src in enumerate(inputs[0]):
        pltpu.make_async_copy(src.at[:, lead], local.at[k, :, lead], lead_sem.at[0]).start()
    for i in (last, *range(last)):
        for a in range(3):
            skip = split if a == 0 else 0
            here = pl.ds(skip, widths[a] - skip)
            there = pl.ds(starts[a] + skip, widths[a] - skip)
            for k, src in enumerate(inputs[a]):
                pltpu.make_async_copy(src.at[part(i), here], local.at[k, part(i), there], in_sem.at[i]).start()
    norm_loads = [
        pltpu.make_async_copy(src, norm_in.at[k], norm_sem.at[k])
        for k, src in enumerate((norm_train, norm_step))
    ]
    for copy in norm_loads:
        copy.start()

    top[...] = jnp.zeros_like(top)
    step = math.gcd(math.gcd(512, split), width - split)

    def compute(i, low, high):
        for c in range(low, high, step):
            cols = slice(c, c + step)
            best = top[:, cols]
            for g in range(CHUNK // 8):
                at = pl.ds(pl.multiple_of(i * CHUNK + g * 8, 8), 8)
                new = stepped(local[0, at, cols], local[1, at, cols], local[2, at, cols])
                fresh[at, cols] = new
                best = jnp.maximum(best, jnp.abs(new))
            top[:, cols] = best

    def lead_chunk(i, carry):
        compute(i, 0, split)
        return carry

    def chunk(i, carry):
        whole = local.at[:, part(i), rest]
        pltpu.make_async_copy(whole, whole, in_sem.at[i]).wait()
        compute(i, split, width)
        return carry

    whole = local.at[:, :, lead]
    pltpu.make_async_copy(whole, whole, lead_sem.at[0]).wait()
    lax.fori_loop(0, rows // CHUNK, lead_chunk, 0)
    mx[0, :, :split] = jnp.max(top[:, :split], axis=0, keepdims=True)

    pl.semaphore_wait(barrier, 7)

    def remote(src, dst, s, d, peer):
        return pltpu.make_async_remote_copy(
            src_ref=src, dst_ref=dst, send_sem=s, recv_sem=d, device_id=peer, device_id_type=MESH
        )

    def spread(source, first, peers, cols, d):
        for k, peer in enumerate(peers):
            remote(
                mx.at[source, :, cols], mx.at[first + k, :, cols], mx_send.at[0], mx_recv.at[d], peer
            ).start()

    def gathered(cols, d):
        three = mx.at[pl.ds(1, 3), :, cols]
        remote(three, three, mx_send.at[0], mx_recv.at[d], plane[0]).wait_recv()

    def ahead(first, last):
        at = pl.ds(first, last - first)
        to = pl.ds(first - (rows - EARLY), last - first)
        for k in range(2):
            remote(fresh.at[at], early.at[k, to], early_send.at[0], early_recv.at[k], plane[k]).start()

    def plane_max(cols):
        mx[4, :, cols] = jnp.maximum(
            jnp.maximum(mx[0, :, cols], mx[1, :, cols]), jnp.maximum(mx[2, :, cols], mx[3, :, cols])
        )

    def line_max(cols):
        factor[:, cols] = jnp.maximum(
            jnp.maximum(mx[4, :, cols], mx[5, :, cols]), jnp.maximum(mx[6, :, cols], mx[7, :, cols])
        )

    spread(0, 1, plane, lead, 0)
    chunk(last, 0)
    ahead(rows - EARLY, rows - EARLY + FIRST)
    lax.fori_loop(0, last, chunk, 0)
    mx[0, :, split:] = jnp.max(top[:, split:], axis=0, keepdims=True)
    spread(0, 1, plane, rest, 1)
    for copy in norm_loads:
        copy.wait()
    norms[m, f] = jnp.zeros_like(norms[m, f])
    norms[m, f, :, : norm_in.shape[2]] = norm_in[0] + norm_in[1]
    mine = norms.at[m, f]
    for peer in plane:
        remote(mine, mine, nm_send.at[0], nm_recv.at[0], peer).start()
    if FIRST < EARLY:
        ahead(rows - EARLY + FIRST, rows)
    gathered(lead, 0)
    plane_max(slice(0, split))
    spread(4, 5, line, lead, 2)
    gathered(rest, 1)
    plane_max(slice(split, width))
    spread(4, 5, line, rest, 3)
    got_nm = norms.at[m, pl.ds(0, 3)]
    remote(got_nm, got_nm, nm_send.at[0], nm_recv.at[0], plane[0]).wait_recv()
    group = norms.at[m, pl.ds(z * 4, 4)]
    for peer in line:
        remote(group, group, nm_send.at[0], nm_recv.at[1], peer).start()
    gathered(lead, 2)
    line_max(slice(0, split))

    def narrow(ref, skip, block, first, last, low=0, high=width):
        def body(i, carry):
            at = pl.ds(pl.multiple_of(first + i * ROWS, ROWS), ROWS)
            here = pl.ds(pl.multiple_of(first - skip + i * ROWS, ROWS), ROWS)
            for c in range(low, high, step):
                cols = slice(c, c + step)
                held[block, at, cols] = (ref[here, cols] / factor[:, cols]).astype(jnp.bfloat16)
            return carry
        lax.fori_loop(0, (last - first) // ROWS, body, 0)

    def go(zz, rr, piece, way, d, peer):
        for first, last, cols in piece:
            block = held.at[zz * 4 + rr, pl.ds(first, last - first), cols]
            remote(block, block, send.at[way], recv.at[d], peer).start()

    def tiles(piece):
        return sum((last - first) // SUB * (cols.size // LANES) for first, last, cols in piece)

    def span(count):
        blocks, down, across = cover(count, n, rows // SUB, width // LANES)
        return held.at[pl.ds(0, blocks), pl.ds(0, down * SUB), pl.ds(0, across * LANES)]

    def got(piece, d, times=1):
        block = span(tiles(piece) * times)
        remote(block, block, send.at[0], recv.at[d], plane[0]).wait_recv()

    def sent(way, count):
        block = span(count)
        remote(block, block, send.at[way], recv.at[0], plane[0]).wait_send()

    def both(first, last):
        return tuple((p, q, c) for p, q, c in zip(first, last, (lead, rest)) if p < q)

    zero, full, late = (0, 0), (rows, rows), (rows - EARLY, rows - EARLY)
    half_a = tuple(tuple((p + e * SUB) // (2 * SUB) * SUB for p in part_a) for e in (0, 1))
    half_b = tuple(p + (rows - p) // (2 * SUB) * SUB for p in part_a)
    piece_a, piece_b, tail_b = both(zero, part_a), both(part_a, full), both(part_a, late)
    for_x = tuple(both(zero, h) for h in half_a)
    for_y = tuple(both(h, part_a) for h in half_a)
    b_for_x, b_for_y = both(part_a, half_b), both(half_b, full)

    hi = z // 2
    z_end, z_mid, z_mid2, z_end2 = 3 * hi, 1 + hi, 2 - hi, 3 - 3 * hi
    is_end = z == z_end
    is_mid = z == z_mid
    near = z_end + z_mid - z
    plane_of = (r, rx, ry, rd)

    def az(zz, to, outward, piece=piece_a):
        go(zz, r, piece, OUT_A if outward else IN_A, AZ + zz, device(to, r))

    def bz(zz, j, to, outward):
        go(zz, plane_of[j], piece_b, OUT_B if outward else IN_B, BZ + zz * 4 + j, device(to, r))

    def got_az(zz):
        got(piece_a, AZ + zz)

    def got_bz(zz, j):
        got(piece_b, BZ + zz * 4 + j)

    def a_own(zz, piece=piece_a):
        go(zz, r, piece, AX_SENT, AX + zz, plane[0])
        go(zz, r, piece, AY_SENT, AY + zz, plane[1])

    def a_forward(zz, odd):
        got(piece_a, AX + zz)
        go(zz, rx, for_y[odd], FY_SENT, DIAG, plane[1])
        got(piece_a, AY + zz)
        go(zz, ry, for_x[odd], FX_SENT, DIAG, plane[0])

    def outset(piece):
        @pl.when(is_end)
        def _():
            az(z_end, z_mid, False, piece)

        @pl.when(is_mid)
        def _():
            az(z_mid, z_mid2, False, piece)
            az(z_mid, z_end, True, piece)

    narrow(fresh, 0, f, 0, low, 0, split)
    outset(piece_a[:1])
    a_own(z, piece_a[:1])
    gathered(rest, 3)
    line_max(slice(split, width))
    narrow(fresh, 0, f, 0, high, split, width)
    outset(piece_a[1:])
    narrow(fresh, 0, f, low, rows, 0, split)
    narrow(fresh, 0, f, high, rows, split, width)
    if tail_b:
        go(z, r, tail_b, BX_SENT, BX, plane[0])
        go(z, r, tail_b, BY_SENT, BY, plane[1])
    a_own(z, piece_a[1:])
    for k, rr in enumerate((rx, ry)):
        remote(early.at[k], early.at[k], early_send.at[0], early_recv.at[k], plane[k]).wait_recv()
        narrow(early.at[k], rows - EARLY, z * 4 + rr, rows - EARLY, rows)
    if tail_b:
        got(tail_b, BX)
        got(tail_b, BY)
    go(z, rx, b_for_y, BY_SENT, BYF, plane[1])
    go(z, ry, b_for_x, BX_SENT, BXF, plane[0])

    @pl.when(is_end)
    def _():
        for j in (0, 1):
            bz(z_end, j, z_mid, False)
        got_az(z_mid)

    @pl.when(is_mid)
    def _():
        for j in (0, 1):
            bz(z_mid, j, z_mid2, False)
            bz(z_mid, j, z_end, True)
        got_az(z_end)
        az(z_end, z_mid2, False)
        got_az(z_mid2)
        az(z_mid2, z_end, True)

    a_own(near)
    got(b_for_x, BXF)
    got(b_for_y, BYF)

    @pl.when(is_end)
    def _():
        for j in (2, 3):
            bz(z_end, j, z_mid, False)

    @pl.when(is_mid)
    def _():
        for j in (2, 3):
            bz(z_mid, j, z_mid2, False)
            bz(z_mid, j, z_end, True)

    a_forward(z, 0)

    @pl.when(is_end)
    def _():
        got_az(z_mid2)

    a_own(z_mid2)

    @pl.when(is_mid)
    def _():
        got_az(z_end2)
        az(z_end2, z_end, True)

    a_forward(near, 1)

    @pl.when(is_mid)
    def _():
        for j in range(4):
            got_bz(z_end, j)
            bz(z_end, j, z_mid2, False)
        for j in range(4):
            got_bz(z_mid2, j)
            bz(z_mid2, j, z_end, True)

    @pl.when(is_end)
    def _():
        got_az(z_end2)

    a_own(z_end2)
    a_forward(z_mid2, 0)

    @pl.when(is_mid)
    def _():
        for j in range(4):
            got_bz(z_end2, j)
            bz(z_end2, j, z_end, True)

    got_nm = norms.at[m, pl.ds(0, 12)]
    remote(got_nm, got_nm, nm_send.at[0], nm_recv.at[1], plane[0]).wait_recv()
    whole = norms.at[m]
    remote(whole, whole, nm_send.at[1], nm_recv.at[2], partner).start()

    a_forward(z_end2, 1)

    @pl.when(is_end)
    def _():
        for zz in (z_mid, z_mid2, z_end2):
            for j in range(4):
                got_bz(zz, j)

    diagonal = span(4 * tiles(piece_a))
    remote(diagonal, diagonal, send.at[0], recv.at[DIAG], plane[0]).wait_recv()
    theirs = norms.at[1 - m]
    remote(theirs, theirs, nm_send.at[1], nm_recv.at[2], partner).wait_recv()
    sums = mx.at[pl.ds(0, 6)]
    remote(sums, sums, mx_send.at[0], mx_recv.at[0], plane[0]).wait_send()
    tags = norms.at[m, pl.ds(0, 15)]
    remote(tags, tags, nm_send.at[0], nm_recv.at[0], plane[0]).wait_send()
    remote(theirs, theirs, nm_send.at[1], nm_recv.at[2], partner).wait_send()
    remote(early, early, early_send.at[0], early_recv.at[0], plane[0]).wait_send()
    sent(AX_SENT, 4 * tiles(piece_a))
    sent(AY_SENT, 4 * tiles(piece_a))
    sent(FX_SENT, 2 * tiles(for_x[0]) + 2 * tiles(for_x[1]))
    sent(FY_SENT, 2 * tiles(for_y[0]) + 2 * tiles(for_y[1]))
    sent(BX_SENT, tiles(tail_b) + tiles(b_for_x))
    sent(BY_SENT, tiles(tail_b) + tiles(b_for_y))

    @pl.when(is_end)
    def _():
        sent(IN_A, tiles(piece_a))
        sent(IN_B, 4 * tiles(piece_b))

    @pl.when(is_mid)
    def _():
        sent(IN_A, 2 * tiles(piece_a))
        sent(IN_B, 8 * tiles(piece_b))
        sent(OUT_A, 3 * tiles(piece_a))
        sent(OUT_B, 12 * tiles(piece_b))


def write_kernel(length, held, fresh, factor, norms, *rest):
    serve, rates, fresh_out, norm_out, flat, norm_row, sems = rest[:3], rest[3:6], rest[6:9], *rest[9:]
    n = held.shape[0]
    cut = max(1, n // 4)
    start = 0
    for k in range(3):
        cols = pl.ds(start, serve[k].shape[2])
        for b in range(0, n, cut):
            pltpu.make_async_copy(held.at[pl.ds(b, cut), :, cols], serve[k].at[pl.ds(b, cut)], sems.at[0]).start()
        pltpu.make_async_copy(fresh.at[:, cols], fresh_out[k], sems.at[1]).start()
        pltpu.make_async_copy(factor.at[:, cols], rates[k], sems.at[2]).start()
        start += serve[k].shape[2]
    at = 0
    for b in range(n):
        for c in range(norms.shape[0]):
            flat[:, at : at + length] = norms[c, b, :, :length]
            at += length
    norm_row[...] = flat[...].astype(jnp.bfloat16).reshape(at)
    last = pltpu.make_async_copy(norm_row, norm_out, sems.at[3])
    last.start()
    for k, whole in enumerate((held, fresh, factor)):
        pltpu.make_async_copy(whole, whole, sems.at[k]).wait()
    last.wait()


def with_kernel(part_a, split, *args):
    (tq, dq, sq, tk, dk, sk, tv, dv, sv, norm_train, norm_step) = args
    length = norm_train.shape[0]
    padded = -(-length // LANES) * LANES
    n, cores = lax.axis_size("fsdp"), lax.axis_size("model")
    rows = tq.shape[0]
    widths = (tq.shape[1], tk.shape[1], tv.shape[1])
    width = sum(widths)
    vmem = pl.BlockSpec(memory_space=pltpu.VMEM)
    hbm = pl.BlockSpec(memory_space=pltpu.HBM)
    f32, bf16 = jnp.float32, jnp.bfloat16
    room = VMEM_BYTES - n * rows * width * 2 - rows * width * 4 - 192 * 1024
    held, fresh, factor, norms = pl.pallas_call(
        functools.partial(gather_kernel, part_a, split, widths),
        out_shape=(
            pltpu.VMEM((n, rows, width), bf16),
            pltpu.VMEM((rows, width), f32),
            pltpu.VMEM((1, width), f32),
            pltpu.VMEM((cores, n, 1, padded), f32),
        ),
        in_specs=[hbm] * 11,
        out_specs=(vmem,) * 4,
        scratch_shapes=[
            pltpu.VMEM((3, rows, width), f32),
            pltpu.VMEM((2, 1, length), f32),
            pltpu.VMEM((8, width), f32),
            pltpu.VMEM((2, EARLY, width), f32),
            pltpu.VMEM((8, 1, width), f32),
            pltpu.SemaphoreType.DMA((1,)),
            pltpu.SemaphoreType.DMA((rows // CHUNK,)),
            pltpu.SemaphoreType.DMA((2,)),
            pltpu.SemaphoreType.DMA((1,)),
            pltpu.SemaphoreType.DMA((4,)),
            pltpu.SemaphoreType.DMA((2,)),
            pltpu.SemaphoreType.DMA((3,)),
            pltpu.SemaphoreType.DMA((1,)),
            pltpu.SemaphoreType.DMA((2,)),
            pltpu.SemaphoreType.DMA((KINDS,)),
            pltpu.SemaphoreType.DMA((COUNT,)),
        ],
        compiler_params=pltpu.CompilerParams(
            collective_id=0, has_side_effects=True, vmem_limit_bytes=room
        ),
        name="gather",
    )(
        tq, dq, sq, tk, dk, sk, tv, dv, sv,
        norm_train.reshape(1, length), norm_step.reshape(1, length),
    )
    out = pl.pallas_call(
        functools.partial(write_kernel, length),
        out_shape=(
            *[jax.ShapeDtypeStruct((n, rows, w), bf16) for w in widths],
            *[jax.ShapeDtypeStruct((1, w), f32) for w in widths],
            *[jax.ShapeDtypeStruct((rows, w), f32) for w in widths],
            jax.ShapeDtypeStruct((n * cores * length,), bf16),
        ),
        in_specs=[vmem] * 4,
        out_specs=(hbm,) * 10,
        scratch_shapes=[
            pltpu.VMEM((1, n * cores * length), f32),
            pltpu.VMEM((n * cores * length,), bf16),
            pltpu.SemaphoreType.DMA((4,)),
        ],
        compiler_params=pltpu.CompilerParams(vmem_limit_bytes=4 * 1024 * 1024),
        name="write",
    )(held, fresh, factor, norms)
    return (
        *[a.reshape(n * rows, w) for a, w in zip(out[:3], widths)],
        *[a.reshape(w) for a, w in zip(out[3:6], widths)],
        out[9], *out[6:9],
    )


def per_device(
    train_query,
    drift_query,
    spread_query,
    train_key,
    drift_key,
    spread_key,
    train_value,
    drift_value,
    spread_value,
    norm_train,
    norm_step,
):
    n, cores, rows = lax.axis_size("fsdp"), lax.axis_size("model"), train_query.shape[0]
    split = LEAD * LANES
    part_a = (rows - rows // SUB // 4 * SUB, rows - rows // SUB // 5 * SUB)
    lanes_ok = all(a.shape[1] % LANES == 0 for a in (train_query, train_key, train_value))
    if n == 16 and cores == 2 and rows % CHUNK == 0 and part_a[1] + EARLY <= rows and lanes_ok:
        return with_kernel(
            part_a, split,
            train_query, drift_query, spread_query,
            train_key, drift_key, spread_key,
            train_value, drift_value, spread_value,
            norm_train, norm_step,
        )
    fresh_query = train_query - learn_rate * (
        drift_query / (jnp.sqrt(spread_query) + tiny_value) + decay_rate * train_query
    )
    fresh_key = train_key - learn_rate * (
        drift_key / (jnp.sqrt(spread_key) + tiny_value) + decay_rate * train_key
    )
    fresh_value = train_value - learn_rate * (
        drift_value / (jnp.sqrt(spread_value) + tiny_value) + decay_rate * train_value
    )
    factor_query, factor_key, factor_value = lax.pmax(
        (
            jnp.max(jnp.abs(fresh_query), axis=0),
            jnp.max(jnp.abs(fresh_key), axis=0),
            jnp.max(jnp.abs(fresh_value), axis=0),
        ),
        "fsdp",
    )
    narrow_query, narrow_key, narrow_value = (
        (fresh_query / factor_query).astype(jnp.bfloat16),
        (fresh_key / factor_key).astype(jnp.bfloat16),
        (fresh_value / factor_value).astype(jnp.bfloat16),
    )
    serve_query, serve_key, serve_value = (
        lax.all_gather(narrow_query, "fsdp", axis=0, tiled=True),
        lax.all_gather(narrow_key, "fsdp", axis=0, tiled=True),
        lax.all_gather(narrow_value, "fsdp", axis=0, tiled=True),
    )
    serve_norm = lax.all_gather(
        (norm_train + norm_step).astype(jnp.bfloat16), ("fsdp", "model"), axis=0, tiled=True
    )
    return (
        serve_query,
        serve_key,
        serve_value,
        factor_query,
        factor_key,
        factor_value,
        serve_norm,
        fresh_query,
        fresh_key,
        fresh_value,
    )


def solution(mesh):
    in_specs = (
        P("fsdp", "model"),
        P("fsdp", "model"),
        P("fsdp", "model"),
        P("fsdp", "model"),
        P("fsdp", "model"),
        P("fsdp", "model"),
        P("fsdp", "model"),
        P("fsdp", "model"),
        P("fsdp", "model"),
        P(("fsdp", "model")),
        P(("fsdp", "model")),
    )
    out_specs = (
        P(None, "model"),
        P(None, "model"),
        P(None, "model"),
        P("model"),
        P("model"),
        P("model"),
        P(),
        P("fsdp", "model"),
        P("fsdp", "model"),
        P("fsdp", "model"),
    )
    return jax.shard_map(
        per_device, mesh=mesh, in_specs=in_specs, out_specs=out_specs, check_vma=False
    )
```
